32 devices in a mesh: gx: 8 (over z, x), gy: 4 (over y, core).
Axes of the slice: x: 2, y: 2, z: 4, core: 2. Of those that a mesh axis runs over, the one named last changes fastest.
Arguments:
- measures: bfloat16 [262144, 128], P(('gx', 'gy')), may hold values from -6 to 6
- row_keys: int32 [262144], P(('gx', 'gy')), may hold values from 0 to 16383, as said below
- orders: bfloat16 [16384, 128], P(('gx', 'gy')), may hold values from -6 to 6
- heavy_keys: int32 [64], replicated, may hold values from 0 to 16383, as said below
- key_slot: int32 [16384], replicated, may hold values from 0 to 16383, as said below
Outputs:
- result: bfloat16 [16384, 128], P(('gx', 'gy'))
- heavy_report: bfloat16 [64, 128], P(('gx', 'gy'))
- slot_rows: float32 [16384], P(('gx', 'gy'))
The draws below stay inside these ranges and needn't reach their ends.
Inputs may be any that keep to these rules, and one draw needn't show every extreme that they name: `heavy_keys`: for each range block d, entries d * 2 to (d + 1) * 2 - 1 are distinct keys of d * 512 to (d + 1) * 512 - 1. `key_slot`: A permutation. Slot s belongs to owner s // 2048 and to quarter (s // 512) % q with q = 4. Key k lies in range block d = k // 512; every range block has exactly 64 keys with slots of each owner, all in quarter d % q. `row_keys`: in the rows of one device, among rows whose key is not heavy, at most 768 have slots of any one owner and at most 192 distinct keys have slots of any one owner; in every device both bounds are reached by some owner.
All inputs are finite; a program needn't handle non-finite values.
Results may differ from the reference program's by a relative error of at most 0.0021.
Values may be sent and summed in bfloat16 or wider, within the bound.
A program may use at most 64 MiB of HBM per device.

```python
import jax
import jax.numpy as jnp
from jax import lax

W = 128
ROWS_DEV = 8192
KEY_DEV = 512
HPD = 2
ROWS = 262144
KEYS = 16384
HEAVY = 64
OWN_SLOTS = 2048
KPP = 64
CAP = 768
CAPK = 192
N_GX = 8
N_GY = 4
DEVICES = 32


def layout(base):
    seeded = jax.random.fold_in(base, 7)
    first, second, third = jax.random.split(seeded, 3)
    owner_perm = jax.vmap(lambda keyone: jax.random.permutation(keyone, KEY_DEV))(jax.random.split(first, DEVICES))
    device = jnp.arange(DEVICES, dtype=jnp.int32)
    along_x = device // N_GY
    along_y = device % N_GY
    owners = owner_perm // KPP
    within = owner_perm % KPP
    shuffle = jax.vmap(lambda keyone: jax.random.permutation(keyone, KEY_DEV))(jax.random.split(second, N_GX * N_GY))
    shuffle = shuffle.reshape(N_GX, N_GY, KEY_DEV)
    position = shuffle[owners, along_y[:, None], along_x[:, None] * KPP + within]
    key_slot = ((owners * N_GY + along_y[:, None]) * KEY_DEV + position).reshape(KEYS).astype(jnp.int32)
    picked = jax.vmap(lambda keyone: jax.random.permutation(keyone, KEY_DEV)[:HPD])(jax.random.split(third, DEVICES))
    heavy_keys = (device[:, None] * KEY_DEV + picked).reshape(HEAVY).astype(jnp.int32)
    slot_to_key = jnp.argsort(key_slot).astype(jnp.int32)
    heavy_flag = jnp.zeros((KEYS,), jnp.int32).at[heavy_keys].set(1)
    heavy_slot = heavy_flag[slot_to_key]
    return (key_slot, heavy_keys, slot_to_key, heavy_slot)


def draw_key_slot(key, part):
    return layout(key)[0]


def draw_heavy_keys(key, part):
    return layout(key)[1]


def draw_row_keys(key, part):
    key_slot, heavy_keys, slot_to_key, heavy_slot = layout(key)
    seeded = jax.random.fold_in(key, 11)
    favored_pool = jax.random.permutation(jax.random.fold_in(seeded, 3), N_GX)[:max(1, N_GX // 16)]
    tickets = N_GX * CAP
    pool_rank = jnp.where(heavy_slot.reshape(N_GX, OWN_SLOTS) == 1, OWN_SLOTS, 0)

    def one_device(keyone):
        parts = jax.random.split(keyone, 7)
        heavy_count = jax.random.randint(parts[0], (), ROWS_DEV // 4, ROWS_DEV // 2 + 1)
        light_count = ROWS_DEV - heavy_count
        favored = favored_pool[jax.random.randint(parts[1], (), 0, favored_pool.shape[0])]
        ticket_owner = jnp.arange(tickets, dtype=jnp.int32) // CAP
        scores = jnp.where(ticket_owner == favored, 0, tickets) + jax.random.permutation(parts[2], tickets)
        ticket_order = jnp.argsort(scores).astype(jnp.int32)
        row_index = jnp.arange(ROWS_DEV, dtype=jnp.int32)
        chosen = ticket_order[jnp.minimum(row_index, tickets - 1)]
        row_owner = chosen // CAP
        row_ticket = chosen % CAP
        mixing = jax.vmap(lambda keytwo: jax.random.permutation(keytwo, OWN_SLOTS))(jax.random.split(parts[3], N_GX))
        pools = jnp.argsort(pool_rank + mixing, axis=1)[:, :CAPK].astype(jnp.int32)
        spare = jax.random.randint(parts[4], (ROWS_DEV,), 0, CAPK)
        pool_index = jnp.where(row_ticket < CAPK, row_ticket, spare)
        light_keys = slot_to_key[row_owner * OWN_SLOTS + pools[row_owner, pool_index]]
        heavy_pick = heavy_keys[jax.random.randint(parts[5], (ROWS_DEV,), 0, HEAVY)]
        chosen_keys = jnp.where(row_index < light_count, light_keys, heavy_pick)
        return chosen_keys[jax.random.permutation(parts[6], ROWS_DEV)]
    return jax.vmap(one_device)(jax.random.split(seeded, DEVICES)).reshape(ROWS).astype(jnp.int32)


def level_of(own_key, dims, cuts, least, largest):
    factor_of = 1.0
    for dim, shards_of in cuts:
        draws = jax.random.uniform(jax.random.fold_in(jax.random.fold_in(own_key, 6), dim), (shards_of,), jnp.float32, least / len(cuts), largest / len(cuts))
        factor_of = factor_of * jnp.repeat(jnp.exp(draws), dims[dim] // shards_of).reshape((-1,) + (1,) * (len(dims) - 1 - dim))
    return factor_of


def scatter_about(rng, dims, spread, reach, pieces=(), kind=jnp.bfloat16):
    gain = level_of(rng, dims, pieces, -0.22, 0.18) if pieces else 1.0
    drawn = jax.random.normal(rng, dims, jnp.float32) * spread * gain
    return jnp.minimum(jnp.maximum(drawn, -reach), reach).astype(kind)


def setup_inputs(seed: int = 0) -> dict:
    key_list = jax.random.split(jax.random.key(seed), 6)
    return {
        "measures": scatter_about(key_list[0], (ROWS, W), 1.0, 6.0, ((0, 32),)),
        "row_keys": draw_row_keys(jax.random.fold_in(key_list[5], 71), 0),
        "orders": scatter_about(key_list[2], (KEYS, W), 1.0, 6.0, ((0, 32),)),
        "heavy_keys": draw_heavy_keys(jax.random.fold_in(key_list[5], 71), 0),
        "key_slot": draw_key_slot(jax.random.fold_in(key_list[5], 71), 0),
    }


def reference(measures, row_keys, orders, heavy_keys, key_slot):
    blocks = measures.reshape(DEVICES, ROWS_DEV, W)
    block_keys = row_keys.reshape(DEVICES, ROWS_DEV)

    def add_block(running, block_piece):
        block_rows, keys_here = block_piece
        totals = running[0] + jax.ops.segment_sum(block_rows.astype(jnp.float32), keys_here, num_segments=KEYS)
        tallies = running[1] + jax.ops.segment_sum(jnp.ones((ROWS_DEV,), jnp.float32), keys_here, num_segments=KEYS)
        return ((totals, tallies), None)
    start_state = (jnp.zeros((KEYS, W), jnp.float32), jnp.zeros((KEYS,), jnp.float32))
    (sums, counts), unused = lax.scan(add_block, start_state, (blocks, block_keys))
    joined = orders.astype(jnp.float32) * sums * lax.rsqrt(1.0 + counts)[:, None]
    result = joined.astype(jnp.bfloat16)
    heavy_report = joined[heavy_keys].astype(jnp.bfloat16)
    heavy_flag = jnp.zeros((KEYS,), jnp.float32).at[heavy_keys].set(1.0)
    slot_rows = jnp.zeros((KEYS,), jnp.float32).at[key_slot].set(counts * (1.0 - heavy_flag))
    return (result, heavy_report, slot_rows)
```

```python
import functools

import jax
import jax.numpy as jnp
from jax import lax
from jax.experimental import pallas as pl
from jax.experimental.pallas import tpu as pltpu
from jax.sharding import PartitionSpec as P

MESH = pl.DeviceIdType.MESH
LANES = 128
F32 = jnp.float32
BF16 = jnp.bfloat16
VMEM = pl.BlockSpec(memory_space=pltpu.VMEM)
ANY = pl.BlockSpec(memory_space=pl.ANY)
SMEM = pl.BlockSpec(memory_space=pltpu.SMEM)
LIMIT = 60 * 1024 * 1024
NN = (((1,), (0,)), ((), ()))
NT = (((1,), (1,)), ((), ()))


def dot(a, b, dims=NN):
    return lax.dot_general(a, b, dims, preferred_element_type=F32)


def iota(shape, dim):
    return lax.broadcasted_iota(jnp.int32, shape, dim)


def onehot(mask):
    return jnp.where(mask, 1.0, 0.0).astype(BF16)


def group_rank(flags, group_rows):
    rows = flags.shape[0]
    lane_r, lane_c = iota((LANES, LANES), 0), iota((LANES, LANES), 1)
    inside = dot(flags, onehot(lane_r < lane_c))
    whole = dot(flags, onehot(lane_r >= 0))
    row_r, row_c = iota((rows, rows), 0), iota((rows, rows), 1)
    earlier = onehot((row_c < row_r) & (row_r // group_rows == row_c // group_rows))
    return inside + dot(earlier, whole.astype(BF16))


def split(values):
    high = values.astype(BF16)
    low = (values - high.astype(F32)).astype(BF16)
    return jnp.concatenate([high, low], axis=1)


def byte_table(table, parts):
    pieces = [((table >> (8 * p)) & 255).astype(F32).T for p in range(parts)]
    return jnp.concatenate(pieces, axis=0).astype(BF16)


def look_up(bytes_table, row_hot, column_mask, parts):
    wide = dot(bytes_table, row_hot)
    found = 0.0
    for p in range(parts):
        piece = wide[p * LANES : (p + 1) * LANES]
        found = found + float(256**p) * jnp.sum(
            jnp.where(column_mask, piece, 0.0), axis=0, keepdims=True
        )
    return found.astype(jnp.int32)


def byte_count(largest):
    return (int(largest).bit_length() + 7) // 8


def gather_rows(cfg, measures, keys, heavy, key_slot, send, tally, small, slots):
    rows, block, nr = cfg["rows"], cfg["block"], cfg["nr"]
    segments, capacity = cfg["segments"], cfg["capacity"]
    slot_parts = byte_count(nr * LANES - 1)
    slot_bytes = byte_table(key_slot[...], slot_parts)
    hist_key = jnp.zeros((nr, LANES), F32)
    hist_slot = jnp.zeros((nr, LANES), F32)
    heavy_sum = jnp.zeros((cfg["heavy"], LANES), F32)
    for c in range(rows // block):
        span = slice(c * block, (c + 1) * block)
        key = keys[:, span]
        row_hot = onehot(iota((nr, block), 0) == key >> 7)
        column_mask = iota((LANES, block), 0) == (key & 127)
        hist_key = hist_key + dot(row_hot, onehot(column_mask), NT)
        heavy_hot = jnp.where(heavy[...] == key, 1.0, 0.0)
        is_heavy = jnp.max(heavy_hot, axis=0, keepdims=True) > 0.0
        heavy_sum = heavy_sum + dot(heavy_hot.astype(BF16), measures[span, :])
        slot = jnp.where(is_heavy, -1, look_up(slot_bytes, row_hot, column_mask, slot_parts))
        slots[:, span] = slot
        slot_row = onehot(iota((nr, block), 0) == slot >> 7)
        slot_column = onehot(iota((LANES, block), 0) == (slot & 127))
        hist_slot = hist_slot + dot(slot_row, slot_column, NT)
    tally[...] = hist_slot
    present = hist_slot > 0.0
    group = cfg["own"] // LANES
    rank = group_rank(onehot(present), group).astype(jnp.int32)
    owner = iota((nr, LANES), 0) // group
    segment_table = jnp.where(present, owner * capacity + rank + 1, 0)
    seg_parts = byte_count(segments)
    segment_bytes = byte_table(segment_table, seg_parts)
    step = cfg["seg_block"]
    for c in range(rows // block):
        span = slice(c * block, (c + 1) * block)
        slot = slots[:, span]
        slot_row = onehot(iota((nr, block), 0) == slot >> 7)
        slot_mask = iota((LANES, block), 0) == (slot & 127)
        segment = look_up(segment_bytes, slot_row, slot_mask, seg_parts) - 1
        for s in range(segments // step):
            hot = onehot(iota((step, block), 0) == segment - s * step)
            product = dot(hot, measures[span, :])
            place = slice(s * step, (s + 1) * step)
            if c == 0:
                send[place, :] = product
            else:
                send[place, :] += product
    each, key_rows, height = cfg["heavy_each"], cfg["key_rows"], cfg["height"]
    small[...] = jnp.zeros(small.shape, F32)
    for d in range(cfg["devices"]):
        small[d * height : d * height + each, :] = heavy_sum[d * each : (d + 1) * each]
        top = (d + 1) * height
        small[top - key_rows : top, :] = hist_key[d * key_rows : (d + 1) * key_rows]


def place_rows(cfg, got, got_tally, key_slot, send, tally, spread, ranks):
    gx, gy, own, kpp = cfg["gx"], cfg["gy"], cfg["own"], cfg["kpp"]
    key_rows, capacity = cfg["key_rows"], cfg["capacity"]
    group = own // LANES
    base = lax.axis_index("gx") * own
    local = key_slot[...] - base
    mine = (local >= 0) & (local < own)
    rank = jnp.where(mine, group_rank(onehot(mine), key_rows), -1.0).astype(jnp.int32)
    local = local.astype(F32)
    for y in range(gy):
        for x in range(gx):
            first = (x * gy + y) * key_rows
            acc = jnp.zeros((kpp, LANES), F32)
            for j in range(key_rows):
                hit = iota((kpp, LANES), 0) == rank[first + j : first + j + 1]
                acc = acc + jnp.where(hit, local[first + j : first + j + 1], 0.0)
            at = (y * gx + x) * kpp
            spread[at : at + kpp, :] = acc
    present = got_tally[...] > 0.0
    ranks[...] = jnp.where(present, group_rank(onehot(present), group) + 1.0, 0.0)
    total = got_tally[0:group]
    for i in range(1, gx):
        total = total + got_tally[i * group : (i + 1) * group]
    tally[...] = total
    values = split(got[...])
    quarter = own // gy
    for q in range(gy):
        at = slice(q * quarter, (q + 1) * quarter)
        slot = jnp.sum(spread[at, :], axis=1, keepdims=True).astype(jnp.int32) - q * quarter
        found = jnp.zeros((quarter, gx), F32)
        for j in range(key_rows):
            hot = onehot(slot - j * LANES == iota((quarter, LANES), 1))
            table = ranks[pl.ds(q * key_rows + j, gx, stride=group), :].astype(BF16)
            found = found + dot(hot, table, NT)
        found = found.astype(jnp.int32) - 1
        out = jnp.zeros((quarter, 2 * LANES), F32)
        for i in range(gx):
            hot = onehot(found[:, i : i + 1] == iota((quarter, capacity), 1))
            out = out + dot(hot, values[i * capacity : (i + 1) * capacity])
        send[at, :] = out[:, :LANES] + out[:, LANES:]


def join_rows(cfg, heavy, got, got_small, got_tally, orders, key_slot, result, report, slot_rows, sums, joined):
    gx, gy, own, kpp = cfg["gx"], cfg["gy"], cfg["own"], cfg["kpp"]
    key_rows, height, each = cfg["key_rows"], cfg["height"], cfg["heavy_each"]
    key_dev = key_rows * LANES
    device = lax.axis_index("gx") * gy + lax.axis_index("gy")
    total = got_tally[0:key_rows]
    for y in range(1, gy):
        total = total + got_tally[y * key_rows : (y + 1) * key_rows]
    slot_rows[...] = total
    small = got_small[0:height]
    for d in range(1, cfg["devices"]):
        small = small + got_small[d * height : (d + 1) * height]
    for x in range(gx):
        first = x * gy * kpp
        part = got[first : first + kpp]
        for y in range(1, gy):
            part = part + got[first + y * kpp : first + (y + 1) * kpp]
        sums[x * kpp : (x + 1) * kpp, :] = part
    values = split(sums[...])
    owner = key_slot[pl.ds(device * key_rows, key_rows), :] // own
    flags = jnp.concatenate([jnp.where(owner == x, 1.0, 0.0) for x in range(gx)], axis=0)
    rank = group_rank(flags.astype(BF16), key_rows)
    place = jnp.zeros((key_rows, LANES), F32)
    for x in range(gx):
        here = rank[x * key_rows : (x + 1) * key_rows] + float(x * kpp)
        place = place + jnp.where(owner == x, here, 0.0)
    counts = small[height - key_rows : height]
    stacked = jnp.concatenate([place, counts], axis=0)
    columns = stacked.T
    for j in range(key_rows):
        at = slice(j * LANES, (j + 1) * LANES)
        where = columns[:, j : j + 1].astype(jnp.int32)
        hot = onehot(where == iota((LANES, key_dev), 1))
        both = dot(hot, values)
        found = both[:, :LANES] + both[:, LANES:]
        for h in range(each):
            spot = heavy[device * each + h] - device * key_dev - j * LANES
            found = found + jnp.where(iota((LANES, LANES), 0) == spot, small[h : h + 1], 0.0)
        scale = lax.rsqrt(1.0 + columns[:, key_rows + j : key_rows + j + 1])
        value = orders[at, :].astype(F32) * found * scale
        joined[at, :] = value
        result[at, :] = value.astype(BF16)
    lines = [
        joined[pl.ds(heavy[device * each + h] - device * key_dev, 1), :] for h in range(each)
    ]
    report[...] = jnp.concatenate(lines, axis=0).astype(BF16)


def all_barrier(gx, gy, me_x, me_y):
    barrier = pltpu.get_barrier_semaphore()
    device = me_x * gy + me_y
    devices = gx * gy

    @pl.loop(1, devices)
    def _(step):
        other = lax.rem(device + step, devices)
        target = (other // gy, lax.rem(other, gy))
        pl.semaphore_signal(barrier, inc=1, device_id=target, device_id_type=MESH)

    pl.semaphore_wait(barrier, devices - 1)


def exchange(me, count, moves, address):
    for source, landing, send_sem, recv_sem, local_sem in moves:
        pltpu.make_async_copy(source(me), landing(me), local_sem).start()

    def remote(other, move):
        source, landing, send_sem, recv_sem, local_sem = move
        return pltpu.make_async_remote_copy(
            src_ref=source(other),
            dst_ref=landing(me),
            send_sem=send_sem.at[other],
            recv_sem=recv_sem.at[me],
            device_id=address(other),
            device_id_type=MESH,
        )

    def finish(other, move):
        source, landing, send_sem, recv_sem, local_sem = move
        copy = pltpu.make_async_remote_copy(
            src_ref=source(other),
            dst_ref=landing(other),
            send_sem=send_sem.at[other],
            recv_sem=recv_sem.at[other],
            device_id=address(other),
            device_id_type=MESH,
        )
        copy.wait_send()
        copy.wait_recv()

    @pl.loop(1, count)
    def _(step):
        for move in moves:
            remote(lax.rem(me + step, count), move).start()

    def end():
        @pl.loop(1, count)
        def _(step):
            for move in moves:
                finish(lax.rem(me + step, count), move)

        for source, landing, send_sem, recv_sem, local_sem in moves:
            pltpu.make_async_copy(source(me), landing(me), local_sem).wait()

    return end


def to_owners(gx, gy, send, tally, small, got, got_tally, got_small, sem_a, sem_b, sem_c, sem_d, sem_e, sem_f, local):
    me_x, me_y = lax.axis_index("gx"), lax.axis_index("gy")
    all_barrier(gx, gy, me_x, me_y)
    rows = (lambda i: send.at[i], lambda i: got.at[i], sem_a, sem_b, local.at[0])
    tallies = (lambda i: tally.at[i], lambda i: got_tally.at[i], sem_c, sem_d, local.at[1])
    end_x = exchange(me_x, gx, [rows, tallies], lambda i: (i, me_y))
    others = (lambda i: small.at[i], lambda i: got_small.at[i], sem_e, sem_f, local.at[2])
    end_all = exchange(
        me_x * gy + me_y, gx * gy, [others], lambda i: (i // gy, lax.rem(i, gy))
    )
    end_x()
    end_all()


def to_ranges(gx, gy, send, tally, got, got_tally, sem_a, sem_b, sem_c, sem_d, local):
    me_x, me_y = lax.axis_index("gx"), lax.axis_index("gy")
    all_barrier(gx, gy, me_x, me_y)
    rows = (
        lambda i: send.at[lax.rem(i, gy) * gx + i // gy],
        lambda i: got.at[i],
        sem_a,
        sem_b,
        local.at[0],
    )
    end_all = exchange(
        me_x * gy + me_y, gx * gy, [rows], lambda i: (i // gy, lax.rem(i, gy))
    )
    tallies = (lambda i: tally.at[i], lambda i: got_tally.at[i], sem_c, sem_d, local.at[1])
    end_y = exchange(me_y, gy, [tallies], lambda i: (me_x, i))
    end_y()
    end_all()


def shaped(*dims, dtype=F32):
    return jax.ShapeDtypeStruct(dims, dtype)


def body(measures, row_keys, orders, heavy_keys, key_slot):
    rows, columns = measures.shape
    gx, gy = lax.axis_size("gx"), lax.axis_size("gy")
    devices = gx * gy
    key_dev = orders.shape[0]
    key_rows = key_dev // LANES
    own = key_dev * gy
    nr = key_slot.shape[0] // LANES
    heavy = heavy_keys.shape[0]
    each = heavy // devices
    capacity = max(rows // 32, 3 * rows // (4 * gx)) // 4
    segments = gx * capacity
    cfg = dict(
        rows=rows,
        block=min(rows, 2048),
        nr=nr,
        gx=gx,
        gy=gy,
        devices=devices,
        own=own,
        kpp=key_dev // gx,
        key_rows=key_rows,
        heavy=heavy,
        heavy_each=each,
        height=-(-(each + key_rows) // 8) * 8,
        capacity=capacity,
        segments=segments,
        seg_block=512 if segments % 512 == 0 else segments,
    )
    height = cfg["height"]
    group = own // LANES
    params = pltpu.CompilerParams(vmem_limit_bytes=LIMIT)
    table = key_slot.reshape(nr, LANES)
    send, tally, small = pl.pallas_call(
        functools.partial(gather_rows, cfg),
        out_shape=(
            shaped(segments, columns),
            shaped(nr, LANES),
            shaped(devices * height, LANES),
        ),
        in_specs=[VMEM] * 4,
        out_specs=(VMEM,) * 3,
        scratch_shapes=[pltpu.VMEM((1, rows), jnp.int32)],
        compiler_params=params,
    )(measures, row_keys.reshape(1, rows), heavy_keys.reshape(heavy, 1), table)
    dma = pltpu.SemaphoreType.DMA
    got, got_tally, got_small = pl.pallas_call(
        functools.partial(to_owners, gx, gy),
        out_shape=(
            shaped(gx, capacity, columns),
            shaped(gx, group, LANES),
            shaped(devices, height, LANES),
        ),
        in_specs=[ANY] * 3,
        out_specs=(ANY,) * 3,
        scratch_shapes=[dma((gx,))] * 4 + [dma((devices,))] * 2 + [dma((3,))],
        compiler_params=pltpu.CompilerParams(collective_id=0, has_side_effects=True),
    )(
        send.reshape(gx, capacity, columns),
        tally.reshape(gx, group, LANES),
        small.reshape(devices, height, LANES),
    )
    send2, tally2 = pl.pallas_call(
        functools.partial(place_rows, cfg),
        out_shape=(shaped(own, columns), shaped(group, LANES)),
        in_specs=[VMEM] * 3,
        out_specs=(VMEM,) * 2,
        scratch_shapes=[pltpu.VMEM((own, LANES), F32), pltpu.VMEM((gx * group, LANES), F32)],
        compiler_params=params,
    )(got.reshape(segments, columns), got_tally.reshape(gx * group, LANES), table)
    got2, got_tally2 = pl.pallas_call(
        functools.partial(to_ranges, gx, gy),
        out_shape=(shaped(devices, cfg["kpp"], columns), shaped(gy, key_rows, LANES)),
        in_specs=[ANY] * 2,
        out_specs=(ANY,) * 2,
        scratch_shapes=[dma((devices,))] * 2 + [dma((gy,))] * 2 + [dma((2,))],
        compiler_params=pltpu.CompilerParams(collective_id=1, has_side_effects=True),
    )(send2.reshape(devices, cfg["kpp"], columns), tally2.reshape(gy, key_rows, LANES))
    result, report, slot_rows = pl.pallas_call(
        functools.partial(join_rows, cfg),
        out_shape=(
            shaped(key_dev, columns, dtype=BF16),
            shaped(each, columns, dtype=BF16),
            shaped(key_rows, LANES),
        ),
        in_specs=[SMEM] + [VMEM] * 5,
        out_specs=(VMEM,) * 3,
        scratch_shapes=[pltpu.VMEM((key_dev, LANES), F32)] * 2,
        compiler_params=params,
    )(
        heavy_keys,
        got2.reshape(devices * cfg["kpp"], columns),
        got_small.reshape(devices * height, LANES),
        got_tally2.reshape(gy * key_rows, LANES),
        orders,
        table,
    )
    return (result, report, slot_rows.reshape(key_dev))


def solution(mesh):
    return jax.shard_map(
        body,
        mesh=mesh,
        in_specs=(P(("gx", "gy"), None), P(("gx", "gy")), P(("gx", "gy"), None), P(), P()),
        out_specs=(P(("gx", "gy"), None), P(("gx", "gy"), None), P(("gx", "gy"))),
        check_vma=False,
    )
```
